32 devices in a mesh: data: 8 (over z, y), width: 4 (over x, core).
Axes of the slice: x: 2, y: 2, z: 4, core: 2. Of those that a mesh axis runs over, the one named last changes fastest.
Arguments:
- grad_up: float32 [8, 768, 3072], P('data', None, 'width'), may hold values from -4 to 4
- grad_down: float32 [8, 3072, 768], P('data', 'width'), may hold values from -4 to 4
- grad_query: float32 [8, 768, 768], P('data', None, 'width'), may hold values from -4 to 4
- grad_key: float32 [8, 768, 768], P('data', None, 'width'), may hold values from -4 to 4
- grad_value: float32 [8, 768, 768], P('data', None, 'width'), may hold values from -4 to 4
- grad_mixed: float32 [8, 768, 768], P('data', 'width'), may hold values from -4 to 4
- grad_norm: float32 [8, 768], P('data'), may hold values from -8 to 8
- weight_up: float32 [768, 3072], P('data', 'width'), may hold values from -0.21875 to 0.21875
- weight_down: float32 [3072, 768], P('width', 'data'), may hold values from -0.109375 to 0.109375
- weight_query: float32 [768, 768], P('data', 'width'), may hold values from -0.21875 to 0.21875
- weight_key: float32 [768, 768], P('data', 'width'), may hold values from -0.21875 to 0.21875
- weight_value: float32 [768, 768], P('data', 'width'), may hold values from -0.21875 to 0.21875
- weight_mixed: float32 [768, 768], P('width', 'data'), may hold values from -0.21875 to 0.21875
- weight_norm: float32 [768], P('data'), may hold values from 0.25 to 1.75
- moment_up: float32 [768, 3072], P('data', 'width'), may hold values from 0.05 to 0.8
- moment_down: float32 [3072, 768], P('width', 'data'), may hold values from 0.05 to 0.8
- moment_query: float32 [768, 768], P('data', 'width'), may hold values from 0.05 to 0.8
- moment_key: float32 [768, 768], P('data', 'width'), may hold values from 0.05 to 0.8
- moment_value: float32 [768, 768], P('data', 'width'), may hold values from 0.05 to 0.8
- moment_mixed: float32 [768, 768], P('width', 'data'), may hold values from 0.05 to 0.8
- moment_norm: float32 [768], P('data'), may hold values from 0.05 to 0.8
Outputs:
- copy_up: bfloat16 [768, 3072], P(None, 'width')
- copy_down: bfloat16 [3072, 768], P('width')
- copy_query: bfloat16 [768, 768], P(None, 'width')
- copy_key: bfloat16 [768, 768], P(None, 'width')
- copy_value: bfloat16 [768, 768], P(None, 'width')
- copy_mixed: bfloat16 [768, 768], P('width')
- copy_norm: bfloat16 [768], replicated
- new_up: float32 [768, 3072], P('data', 'width')
- new_down: float32 [3072, 768], P('width', 'data')
- new_query: float32 [768, 768], P('data', 'width')
- new_key: float32 [768, 768], P('data', 'width')
- new_value: float32 [768, 768], P('data', 'width')
- new_mixed: float32 [768, 768], P('width', 'data')
- new_norm: float32 [768], P('data')
- state_new_up: float32 [768, 3072], P('data', 'width')
- state_new_down: float32 [3072, 768], P('width', 'data')
- state_new_query: float32 [768, 768], P('data', 'width')
- state_new_key: float32 [768, 768], P('data', 'width')
- state_new_value: float32 [768, 768], P('data', 'width')
- state_new_mixed: float32 [768, 768], P('width', 'data')
- state_new_norm: float32 [768], P('data')
The draws below stay inside these ranges and needn't reach their ends.
All inputs are finite; a program needn't handle non-finite values.
Results may differ from the reference program's by a relative error of at most 0.0004.
Values may be sent and summed in bfloat16 or wider, within the bound.
A program may use at most 128 MiB of HBM per device.

```python
import jax
import jax.numpy as jnp
from jax import lax

WIDTH = 768
INNER = 3072
ATTN = 768
REPLICAS = 8


def raised(entries, stream_key, source, target, parts, factor):
    owner, partner = [(jnp.arange(entries.shape[axis_at]) // (entries.shape[axis_at] // parts)).reshape([-1 if axis == axis_at else 1 for axis in range(entries.ndim)]) for axis_at in (source, target)]
    chosen = jax.random.permutation(stream_key, parts)[partner]
    strong = (owner == chosen) | (owner == (partner + parts // 2) % parts)
    return jnp.where(strong, factor * entries, entries)


def block_scale(key, dims, split, smallest, largest):
    def one(dim, shards_of):
        draws = jax.random.uniform(jax.random.fold_in(jax.random.fold_in(key, 6), dim), (shards_of,), jnp.float32, smallest / len(split), largest / len(split))
        return jnp.repeat(jnp.exp(draws), dims[dim] // shards_of).reshape((-1,) + (1,) * (len(dims) - dim - 1))

    loudness = one(*split[0])
    for cut in split[1:]:
        loudness = loudness * one(*cut)
    return loudness


def scatter_about(own_key, extent, deviation, reach, split=(), held_as=jnp.bfloat16):
    factor_of = block_scale(own_key, extent, split, -0.22, 0.18) if split else 1.0
    drawn = jax.random.normal(own_key, extent, jnp.float32) * deviation * factor_of
    return jnp.minimum(jnp.maximum(drawn, -reach), reach).astype(held_as)


def noise_with(rng, dims, width, reach, pieces, heavy, kind=jnp.bfloat16):
    drawn = width * jax.random.normal(rng, dims, jnp.float32)
    if pieces:
        drawn = drawn * block_scale(rng, dims, pieces, -0.22, 0.18)
    return jnp.clip(raised(drawn, jax.random.fold_in(rng, 3), *heavy), -reach, reach).astype(kind)


def setup_inputs(seed: int = 0) -> dict:
    keys = jax.random.split(jax.random.key(seed), 22)
    grad_up = noise_with(keys[0], (REPLICAS, WIDTH, INNER), 0.5, 4.0, ((0, 8), (2, 4)), (0, 1, 8, 2.0), jnp.float32)
    grad_down = noise_with(keys[1], (REPLICAS, INNER, WIDTH), 0.5, 4.0, ((0, 8), (1, 4)), (0, 2, 8, 2.0), jnp.float32)
    grad_query = noise_with(keys[2], (REPLICAS, WIDTH, ATTN), 0.5, 4.0, ((0, 8), (2, 4)), (0, 1, 8, 2.0), jnp.float32)
    grad_key = noise_with(keys[3], (REPLICAS, WIDTH, ATTN), 0.5, 4.0, ((0, 8), (2, 4)), (0, 1, 8, 2.0), jnp.float32)
    grad_value = noise_with(keys[4], (REPLICAS, WIDTH, ATTN), 0.5, 4.0, ((0, 8), (2, 4)), (0, 1, 8, 2.0), jnp.float32)
    grad_mixed = noise_with(keys[5], (REPLICAS, ATTN, WIDTH), 0.5, 4.0, ((0, 8), (1, 4)), (0, 2, 8, 2.0), jnp.float32)
    grad_norm = noise_with(keys[6], (REPLICAS, WIDTH), 1.0, 8.0, ((0, 8),), (0, 1, 8, 2.0), jnp.float32)
    weight_up = scatter_about(keys[7], (WIDTH, INNER), WIDTH ** -0.5, 0.21875, ((0, 8), (1, 4)), jnp.float32)
    weight_down = scatter_about(keys[8], (INNER, WIDTH), INNER ** -0.5, 0.109375, ((0, 4), (1, 8)), jnp.float32)
    weight_query = scatter_about(keys[9], (WIDTH, ATTN), WIDTH ** -0.5, 0.21875, ((0, 8), (1, 4)), jnp.float32)
    weight_key = scatter_about(keys[10], (WIDTH, ATTN), WIDTH ** -0.5, 0.21875, ((0, 8), (1, 4)), jnp.float32)
    weight_value = scatter_about(keys[11], (WIDTH, ATTN), WIDTH ** -0.5, 0.21875, ((0, 8), (1, 4)), jnp.float32)
    weight_mixed = scatter_about(keys[12], (ATTN, WIDTH), ATTN ** -0.5, 0.21875, ((0, 4), (1, 8)), jnp.float32)
    weight_norm = jnp.clip(1.0 + 0.15 * jax.random.normal(keys[13], (WIDTH,), jnp.float32), 0.25, 1.75)
    moment_up = jnp.clip(0.05 + 0.75 * jax.random.uniform(keys[14], (WIDTH, INNER), jnp.float32) ** block_scale(keys[14], (WIDTH, INNER), ((0, 8), (1, 4)), -0.2, 0.2), 0.05, 0.8)
    moment_down = jnp.clip(0.05 + 0.75 * jax.random.uniform(keys[15], (INNER, WIDTH), jnp.float32) ** block_scale(keys[15], (INNER, WIDTH), ((0, 4), (1, 8)), -0.2, 0.2), 0.05, 0.8)
    moment_query = jnp.clip(0.05 + 0.75 * jax.random.uniform(keys[16], (WIDTH, ATTN), jnp.float32) ** block_scale(keys[16], (WIDTH, ATTN), ((0, 8), (1, 4)), -0.2, 0.2), 0.05, 0.8)
    moment_key = jnp.clip(0.05 + 0.75 * jax.random.uniform(keys[17], (WIDTH, ATTN), jnp.float32) ** block_scale(keys[17], (WIDTH, ATTN), ((0, 8), (1, 4)), -0.2, 0.2), 0.05, 0.8)
    moment_value = jnp.clip(0.05 + 0.75 * jax.random.uniform(keys[18], (WIDTH, ATTN), jnp.float32) ** block_scale(keys[18], (WIDTH, ATTN), ((0, 8), (1, 4)), -0.2, 0.2), 0.05, 0.8)
    moment_mixed = jnp.clip(0.05 + 0.75 * jax.random.uniform(keys[19], (ATTN, WIDTH), jnp.float32) ** block_scale(keys[19], (ATTN, WIDTH), ((0, 4), (1, 8)), -0.2, 0.2), 0.05, 0.8)
    moment_norm = jnp.clip(0.05 + 0.75 * jax.random.uniform(keys[20], (WIDTH,), jnp.float32) ** block_scale(keys[20], (WIDTH,), ((0, 8),), -0.2, 0.2), 0.05, 0.8)
    return dict(grad_up=grad_up, grad_down=grad_down, grad_query=grad_query, grad_key=grad_key, grad_value=grad_value, grad_mixed=grad_mixed, grad_norm=grad_norm, weight_up=weight_up, weight_down=weight_down, weight_query=weight_query, weight_key=weight_key, weight_value=weight_value, weight_mixed=weight_mixed, weight_norm=weight_norm, moment_up=moment_up, moment_down=moment_down, moment_query=moment_query, moment_key=moment_key, moment_value=moment_value, moment_mixed=moment_mixed, moment_norm=moment_norm)


learn_rate = 0.05
hold_rate = 0.9

def reference(grad_up, grad_down, grad_query, grad_key, grad_value, grad_mixed, grad_norm, weight_up, weight_down, weight_query, weight_key, weight_value, weight_mixed, weight_norm, moment_up, moment_down, moment_query, moment_key, moment_value, moment_mixed, moment_norm):
    mean_up = lax.optimization_barrier(jnp.sum(grad_up.astype(jnp.float32), axis=0)) * REPLICAS ** (-0.5)
    mean_down = lax.optimization_barrier(jnp.sum(grad_down.astype(jnp.float32), axis=0)) * REPLICAS ** (-0.5)
    mean_query = lax.optimization_barrier(jnp.sum(grad_query.astype(jnp.float32), axis=0)) * REPLICAS ** (-0.5)
    mean_key = lax.optimization_barrier(jnp.sum(grad_key.astype(jnp.float32), axis=0)) * REPLICAS ** (-0.5)
    mean_value = lax.optimization_barrier(jnp.sum(grad_value.astype(jnp.float32), axis=0)) * REPLICAS ** (-0.5)
    mean_mixed = lax.optimization_barrier(jnp.sum(grad_mixed.astype(jnp.float32), axis=0)) * REPLICAS ** (-0.5)
    mean_norm = lax.optimization_barrier(jnp.sum(grad_norm.astype(jnp.float32), axis=0)) * REPLICAS ** (-0.5)
    state_new_up = hold_rate * moment_up + (1.0 - hold_rate) * mean_up * mean_up
    new_up = weight_up - learn_rate * mean_up * lax.rsqrt(state_new_up + 1e-06)
    state_new_down = hold_rate * moment_down + (1.0 - hold_rate) * mean_down * mean_down
    new_down = weight_down - learn_rate * mean_down * lax.rsqrt(state_new_down + 1e-06)
    state_new_query = hold_rate * moment_query + (1.0 - hold_rate) * mean_query * mean_query
    new_query = weight_query - learn_rate * mean_query * lax.rsqrt(state_new_query + 1e-06)
    state_new_key = hold_rate * moment_key + (1.0 - hold_rate) * mean_key * mean_key
    new_key = weight_key - learn_rate * mean_key * lax.rsqrt(state_new_key + 1e-06)
    state_new_value = hold_rate * moment_value + (1.0 - hold_rate) * mean_value * mean_value
    new_value = weight_value - learn_rate * mean_value * lax.rsqrt(state_new_value + 1e-06)
    state_new_mixed = hold_rate * moment_mixed + (1.0 - hold_rate) * mean_mixed * mean_mixed
    new_mixed = weight_mixed - learn_rate * mean_mixed * lax.rsqrt(state_new_mixed + 1e-06)
    state_new_norm = hold_rate * moment_norm + (1.0 - hold_rate) * mean_norm * mean_norm
    new_norm = weight_norm - learn_rate * mean_norm * lax.rsqrt(state_new_norm + 1e-06)
    copy_up = new_up.astype(jnp.bfloat16)
    copy_down = new_down.astype(jnp.bfloat16)
    copy_query = new_query.astype(jnp.bfloat16)
    copy_key = new_key.astype(jnp.bfloat16)
    copy_value = new_value.astype(jnp.bfloat16)
    copy_mixed = new_mixed.astype(jnp.bfloat16)
    copy_norm = new_norm.astype(jnp.bfloat16)
    return (copy_up, copy_down, copy_query, copy_key, copy_value, copy_mixed, copy_norm, new_up, new_down, new_query, new_key, new_value, new_mixed, new_norm, state_new_up, state_new_down, state_new_query, state_new_key, state_new_value, state_new_mixed, state_new_norm)
```

```python
import functools

import jax
import jax.numpy as jnp
from jax import lax
from jax.experimental import pallas as pl
from jax.experimental.pallas import tpu as pltpu
from jax.sharding import PartitionSpec as P

learn_rate = 0.05
hold_rate = 0.9
LANES = 128
SUB = 8
LOW, REACH = -125.0, 251.0
TINY = 1e-30


def round_up(value, unit):
    return -(-value // unit) * unit


def turn(block):
    rows, cols = block.shape
    tall, wide = round_up(rows, LANES), round_up(cols, LANES)
    if wide != cols:
        block = jnp.concatenate([block, jnp.zeros((rows, wide - cols), block.dtype)], axis=1)
    if tall != rows:
        block = jnp.concatenate([block, jnp.zeros((tall - rows, wide), block.dtype)], axis=0)
    return block.T[:cols, :rows]


def encode(x):
    limit = jnp.maximum(jnp.max(jnp.abs(x), axis=0, keepdims=True), TINY)
    size = jnp.exp2(jnp.abs(x) * (REACH / limit) + LOW)
    return jnp.where(x < 0.0, -size, size).astype(jnp.bfloat16), limit


def decode(code, limit):
    code = code.astype(jnp.float32)
    rate = limit * (1.0 / REACH)
    size = jnp.log2(jnp.abs(code)) * rate - LOW * rate
    return jnp.where(code < 0.0, -size, size)


def make_chunks(cols, heads):
    pieces = 3 if cols % (3 * LANES) == 0 else 1
    wide = cols // pieces
    up = [("up", i * wide, wide) for i in range(pieces)]
    down = [("down", i * wide, wide) for i in range(pieces)]
    first = [(up[0], True), (("vm", 0, 2 * heads), False)]
    rest = []
    for i in range(pieces):
        rest.append((down[i], i != 1))
        if i + 1 < pieces:
            rest.append((up[i + 1], i != 0))
    rest.insert(3, (("qk", 0, 2 * heads), True))
    return [c + (y, y) for c, y in first + rest]


def kernel(n, chunks, *refs):
    refs = list(refs)
    take = lambda count: [refs.pop(0) for _ in range(count)]
    grads = dict(zip(("up", "down", "query", "key", "value", "mixed", "norm"), take(7)))
    given = take(14)
    c_up, c_down, c_query, c_key, c_value, c_mixed, c_norm = take(7)
    n_up, n_down, n_query, n_key, n_value, n_mixed, n_norm = take(7)
    s_up, s_down, s_query, s_key, s_value, s_mixed, s_norm = take(7)
    near = take(14)
    w_up, w_down, w_query, w_key, w_value, w_mixed, w_norm = near[:7]
    m_up, m_down, m_query, m_key, m_value, m_mixed, m_norm = near[7:]
    count = len(chunks)
    L = n // 2
    raw = take(count)
    part = take(count)
    ysend = take(count)
    yhold = take(count)
    zsend = take(count)
    zhold = take(count)
    ysend_range, yhold_range, zsend_range, zhold_range = take(count), take(count), take(count), take(count)
    copies = take(count)
    g_norm, norm_hold, norm_copy = take(3)
    load_sem, y_sems, z_sems, ag_sems, ay_sems, norm_sems = take(6)

    rows = part[0].shape[-2]
    heads = w_query.shape[-1]
    mean_rate = n ** (-0.5)
    me = lax.axis_index("data")
    y, z = me % 2, me // 2
    other = 1 - y
    partner = me + 1 - 2 * y
    has_left, has_right = z > 0, z < L - 1

    def sources(chunk):
        kind, start, wide = chunks[chunk][:3]
        if kind == "up":
            return [(grads["up"].at[:, :, pl.ds(start, wide)], part[chunk])]
        if kind == "down":
            return [(grads["down"].at[pl.ds(start, wide)], raw[chunk])]
        pair = ("query", "key") if kind == "qk" else ("value", "mixed")
        return [(grads[p], raw[chunk].at[pl.ds(i * heads, heads)]) for i, p in enumerate(pair)]

    loads, small, at = [], [], 0
    for chunk in range(count):
        group = []
        for src, dst in sources(chunk):
            group.append(pltpu.make_async_copy(src, dst, load_sem.at[at]))
            at += 1
        loads.append(group)
    for src, dst in [(grads["norm"], g_norm)] + list(zip(given, near)):
        small.append(pltpu.make_async_copy(src, dst, load_sem.at[at]))
        at += 1
    for group in loads[:2]:
        for load in group:
            load.start()
    small[0].start()
    for group in loads[2:]:
        for load in group:
            load.start()
    for load in small[1:]:
        load.start()

    def start(copies):
        for copy in copies:
            copy.start()

    def wait_recv(copies):
        for copy in copies:
            copy.wait_recv()

    def wait_send(copies):
        for copy in copies:
            copy.wait_send()

    def remote(src, dst, sems, slot, there):
        return pltpu.make_async_remote_copy(
            src_ref=src,
            dst_ref=dst,
            send_sem=sems.at[(0,) + slot],
            recv_sem=sems.at[(1,) + slot],
            device_id={"data": there},
            device_id_type=pl.DeviceIdType.MESH,
        )

    barrier = pltpu.get_barrier_semaphore()
    for step in range(1, n):
        pl.semaphore_signal(
            barrier, inc=1, device_id={"data": (me + step) % n}, device_id_type=pl.DeviceIdType.MESH
        )

    def target(i):
        ahead = L - 1 - z
        far = jnp.where(i < ahead, L - 1 - i, i - ahead)
        back = jnp.where(i < z, i, L - 1 - (i - z))
        return jnp.where(2 * z < L, far, back)

    def y_first(chunk):
        return chunks[chunk][3]

    def y_last(chunk):
        return chunks[chunk][4]

    def prep(chunk):
        for load in loads[chunk]:
            load.wait()
        if chunks[chunk][0] == "up":
            return
        wide = chunks[chunk][2]
        for j in range(wide // LANES):
            block = turn(raw[chunk][j * LANES : (j + 1) * LANES, :])
            part[chunk][:, :, j * LANES : (j + 1) * LANES] = block.reshape(n, rows, LANES)

    def y_copy(chunk, slot):
        pairs = ((ysend, yhold), (ysend_range, yhold_range))
        return [
            remote(src[chunk].at[slot], dst[chunk].at[slot], y_sems, (k, chunk, slot), partner)
            for k, (src, dst) in enumerate(pairs)
        ]

    def y_value(chunk, slot):
        return decode(yhold[chunk][slot], yhold_range[chunk][slot])

    def y_code(chunk, slot, value):
        ysend[chunk][slot], ysend_range[chunk][slot] = encode(value)
        start(y_copy(chunk, slot))

    def start_y(chunk, i):
        t = z if i == L - 1 else target(i)
        y_code(chunk, t, part[chunk][2 * t + other])

    def z_copy(chunk, t):
        right = t > z
        there = jnp.where(right, z + 1, z - 1)
        slot = jnp.where(jnp.logical_and(t < z, t == z - 1), L, t)
        pairs = ((zsend, zhold), (zsend_range, zhold_range))
        return [
            pltpu.make_async_remote_copy(
                src_ref=src[chunk].at[t],
                dst_ref=dst[chunk].at[slot],
                send_sem=z_sems.at[0, k, chunk, t],
                recv_sem=z_sems.at[1, k, chunk, slot],
                device_id={"data": 2 * there + y},
                device_id_type=pl.DeviceIdType.MESH,
            )
            for k, (src, dst) in enumerate(pairs)
        ]

    def z_wait(chunk, slot):
        wait_recv(
            [
                remote(hold[chunk].at[slot], hold[chunk].at[slot], z_sems, (k, chunk, slot), partner)
                for k, hold in enumerate((zhold, zhold_range))
            ]
        )

    def z_value(chunk, slot, k):
        return decode(zhold[chunk][slot, k], zhold_range[chunk][slot, k])

    def step_z(chunk, i):
        t = target(i)
        held = jnp.logical_or(jnp.logical_and(t > z, has_left), jnp.logical_and(t < z, has_right))
        if y_first(chunk):
            wait_recv(y_copy(chunk, t))
            part[chunk][2 * t + y] = part[chunk][2 * t + y] + y_value(chunk, t)
            owners = (2 * t + y,)
        else:
            owners = (2 * t, 2 * t + 1)

        @pl.when(held)
        def _():
            z_wait(chunk, t)
            for k, owner in enumerate(owners):
                total = part[chunk][owner] + z_value(chunk, t, k)
                zsend[chunk][t, k], zsend_range[chunk][t, k] = encode(total)

        @pl.when(jnp.logical_not(held))
        def _():
            for k, owner in enumerate(owners):
                zsend[chunk][t, k], zsend_range[chunk][t, k] = encode(part[chunk][owner])

        start(z_copy(chunk, t))

    def add_held(chunk, owners):
        for k, owner in enumerate(owners):
            for there, slot in ((has_left, z), (has_right, L)):

                @pl.when(there)
                def _():
                    if k == 0:
                        z_wait(chunk, slot)
                    part[chunk][owner] = part[chunk][owner] + z_value(chunk, slot, k)

    def half_z(chunk):
        add_held(chunk, (2 * z, 2 * z + 1))
        y_code(chunk, 0, part[chunk][2 * z + other])

    def update(total, weight, moment):
        mean = total * mean_rate
        state = hold_rate * moment + (1.0 - hold_rate) * mean * mean
        return weight - learn_rate * mean * lax.rsqrt(state + 1e-06), state

    def finish(chunk):
        kind, start, wide = chunks[chunk][:3]
        if y_first(chunk):
            add_held(chunk, (me,))
        slot = z if y_first(chunk) else 0
        wait_recv(y_copy(chunk, slot))
        own = part[chunk][me] + y_value(chunk, slot)
        cols = slice(start, start + wide)
        if kind in ("up", "down"):
            weight, moment, new_out, state_out = (
                (w_up, m_up, n_up, s_up) if kind == "up" else (w_down, m_down, n_down, s_down)
            )
            new, state = update(own, weight[:, cols], moment[:, cols])
            copies[chunk][z, y] = new.astype(jnp.bfloat16)
            new_out[:, cols] = new
            state_out[:, cols] = state
        elif kind == "qk":
            weight = jnp.concatenate([w_query[...], w_key[...]], axis=1)
            moment = jnp.concatenate([m_query[...], m_key[...]], axis=1)
            new, state = update(own, weight, moment)
            copies[chunk][z, y] = new.astype(jnp.bfloat16)
            n_query[...], n_key[...] = new[:, :heads], new[:, heads:]
            s_query[...], s_key[...] = state[:, :heads], state[:, heads:]
        else:
            weight = jnp.concatenate([w_value[...], turn(w_mixed[...])], axis=1)
            moment = jnp.concatenate([m_value[...], turn(m_mixed[...])], axis=1)
            new, state = update(own, weight, moment)
            copies[chunk][z, y] = new.astype(jnp.bfloat16)
            n_value[...], s_value[...] = new[:, :heads], state[:, :heads]
            n_mixed[...] = turn(new[:, heads:])
            s_mixed[...] = turn(state[:, heads:])
        if y_last(chunk):
            spread(chunk, z, True, True)
            share(chunk, z).start()
        else:
            pair_copy(chunk).start()

    def pair_copy(chunk):
        spot = copies[chunk].at[z, y]
        return remote(spot, spot, ay_sems, (chunk, 0), partner)

    def share(chunk, s):
        spot = copies[chunk].at[s, y]
        return remote(spot, spot, ay_sems, (chunk, s), partner)

    def share_wait(chunk, s):
        spot = copies[chunk].at[s, other]
        remote(spot, spot, ay_sems, (chunk, s), partner).wait_recv()

    def line(chunk, s, right, slot):
        spot = copies[chunk].at[s, y] if y_last(chunk) else copies[chunk].at[s]
        there = z + 1 if right else z - 1
        return pltpu.make_async_remote_copy(
            src_ref=spot,
            dst_ref=spot,
            send_sem=ag_sems.at[0, chunk, slot],
            recv_sem=ag_sems.at[1, chunk, s],
            device_id={"data": 2 * there + y},
            device_id_type=pl.DeviceIdType.MESH,
        )

    def spread(chunk, s, right, left):
        if right:

            @pl.when(has_right)
            def _():
                line(chunk, s, True, s).start()

        if left:

            @pl.when(has_left)
            def _():
                line(chunk, s, False, L if right else s).start()

    def start_pair(chunk):
        spot = copies[chunk].at[z, other]
        remote(spot, spot, ay_sems, (chunk, 0), partner).wait_recv()
        spread(chunk, z, True, True)

    def hop(chunk, h):
        for right in (True, False):
            s = z - h if right else z + h

            @pl.when(s >= 0 if right else s < L)
            def _():
                line(chunk, s, right, s).wait_recv()
                spread(chunk, s, right, not right)
                if y_last(chunk):
                    share(chunk, s).start()

    def drain_reduce(chunk):
        for t in range(L if y_first(chunk) else 1):
            wait_send(y_copy(chunk, t))
        for i in range(L - 1):
            wait_send(z_copy(chunk, target(i)))

    def drain_gather(chunk):
        if y_last(chunk):
            for s in range(L):
                share(chunk, s).wait_send()
        else:
            pair_copy(chunk).wait_send()

        @pl.when(has_right)
        def _():
            line(chunk, z, True, z).wait_send()

        @pl.when(has_left)
        def _():
            line(chunk, z, False, L).wait_send()

        for h in range(1, L):

            @pl.when(jnp.logical_and(z - h >= 0, has_right))
            def _():
                line(chunk, z - h, True, z - h).wait_send()

            @pl.when(jnp.logical_and(z + h < L, has_left))
            def _():
                line(chunk, z + h, False, z + h).wait_send()

    group = 1 if rows % 16 == 0 else 2

    def end(chunk):
        kind, start, wide = chunks[chunk][:3]
        if y_last(chunk):
            for s in range(L):
                share_wait(chunk, s)
        if kind == "up":
            for d in range(0, n, group):
                got = [copies[chunk][(d + i) // 2, (d + i) % 2] for i in range(group)]
                if group > 1:
                    got = [jnp.concatenate([g.astype(jnp.float32) for g in got], axis=0).astype(jnp.bfloat16)]
                c_up[d * rows : (d + group) * rows, start : start + wide] = got[0]
            return
        for j in range(wide // LANES):
            value = copies[chunk][:, :, :, j * LANES : (j + 1) * LANES].astype(jnp.float32)
            value = turn(value.reshape(n * rows, LANES)).astype(jnp.bfloat16)
            if kind == "down":
                c_down[start + j * LANES : start + (j + 1) * LANES, :] = value
                continue
            first, second = (c_query, c_key) if kind == "qk" else (c_value, c_mixed)
            done = 0
            while done < LANES:
                at = j * LANES + done
                out, base = (first, 0) if at < heads else (second, heads)
                size = min(LANES - done, heads + base - at)
                out[at - base : at - base + size, :] = value[done : done + size]
                done += size

    def norm_copies(give):
        src, dst = (g_norm, norm_hold) if give else (norm_copy.at[me], norm_copy)
        return [
            remote(src, dst.at[me], norm_sems, (0 if give else 1, step), (me + step) % n) for step in range(1, n)
        ]

    def norm_arrivals(give):
        hold = norm_hold if give else norm_copy
        for step in range(1, n):
            spot = hold.at[(me + n - step) % n]
            remote(spot, spot, norm_sems, (0 if give else 1, step), partner).wait_recv()

    def norm_start():
        small[0].wait()
        norm_hold[me] = g_norm[...]
        for copy in norm_copies(True):
            copy.start()

    def norm_update():
        norm_arrivals(True)
        total = norm_hold[0]
        for d in range(1, n):
            total = total + norm_hold[d]
        own = total[:, :rows]
        for d in range(1, n):
            own = jnp.where(me == d, total[:, d * rows : (d + 1) * rows], own)
        new, state = update(own, w_norm[...], m_norm[...])
        n_norm[...] = new
        s_norm[...] = state
        wide = norm_copy.shape[-1]
        if wide != rows:
            new = jnp.concatenate([new, jnp.zeros((1, wide - rows), jnp.float32)], axis=1)
        norm_copy[me] = new
        for copy in norm_copies(False):
            copy.start()

    def norm_end():
        norm_arrivals(False)
        got = [norm_copy[d][:, :rows] for d in range(n)]
        c_norm[...] = jnp.concatenate(got, axis=1)
        for give in (True, False):
            for copy in norm_copies(give):
                copy.wait_send()

    def smalls():
        for load in small[1:]:
            load.wait()

    events = []
    add = lambda time, body, *args: events.append((time, len(events), body, args))
    gap, hop_time = 4.0, 2.5
    for chunk in range(count):
        time = gap * chunk
        add(time, prep, chunk)
        if y_first(chunk):
            for i in range(L):
                add(time, start_y, chunk, i)
            time += hop_time
        for i in range(L - 1):
            add(time + hop_time * min(i, L // 2), step_z, chunk, i)
        time += hop_time * (L - 1)
        if not y_first(chunk):
            add(time, half_z, chunk)
            time += hop_time
        add(time, finish, chunk)
        if not y_last(chunk):
            time += hop_time
            add(time, start_pair, chunk)
        for h in range(1, L):
            time += hop_time
            add(time, hop, chunk, h)
        add(time, drain_reduce, chunk)
        if y_last(chunk):
            time += hop_time
        add(time, end, chunk)
        add(time + 2 * hop_time, drain_gather, chunk)
    add(gap + 0.1, norm_start)
    add(2 * hop_time, smalls)
    add(gap * 2 + 2 * hop_time, norm_update)
    add(gap * 4 + 2 * hop_time, norm_end)
    events.sort(key=lambda e: e[:2])

    barrier_done = False
    for _, _, body, args in events:
        if body is not prep and not barrier_done:
            pl.semaphore_wait(barrier, n - 1)
            barrier_done = True
        body(*args)


def hand_on(count, *refs):
    given, out, sem = refs[:count], refs[count : 2 * count], refs[2 * count]
    writes = [pltpu.make_async_copy(given[i], out[i], sem.at[i]) for i in range(count)]
    for write in writes:
        write.start()
    for write in writes:
        write.wait()


def solution(mesh):
    n = mesh.shape["data"]
    L = n // 2

    def on_device(*args):
        grads, weights, moments = args[:7], args[7:14], args[14:]
        rows = weights[0].shape[0]
        cols = grads[0].shape[2]
        grads = [g[0].T if i in (2, 3, 4) else g[0] for i, g in enumerate(grads[:6])] + [grads[6]]
        grads[0] = grads[0].reshape(n, rows, cols)
        heads = grads[2].shape[0]
        weights = list(weights[:6]) + [weights[6].reshape(1, rows)]
        moments = list(moments[:6]) + [moments[6].reshape(1, rows)]
        weights[1], moments[1] = weights[1].T, moments[1].T
        chunks = make_chunks(cols, heads)
        count = len(chunks)
        wide_norm = round_up(rows, LANES)
        copy_shapes = [(n * rows, cols), grads[1].shape] + [g.shape for g in grads[2:6]]
        out_shape = (
            [pltpu.VMEM(s, jnp.bfloat16) for s in copy_shapes]
            + [pltpu.VMEM((1, n * rows), jnp.float32)]
            + [pltpu.VMEM(w.shape, jnp.float32) for w in weights] * 2
        )
        scratch = [pltpu.VMEM(w.shape, jnp.float32) for w in weights + moments]
        bf16 = jnp.bfloat16
        scratch += [pltpu.VMEM((c[2], n * rows) if c[0] != "up" else (SUB, LANES), jnp.float32) for c in chunks]
        scratch += [pltpu.VMEM((n, rows, c[2]), jnp.float32) for c in chunks]
        for tall, dtype in ((rows, bf16), (1, jnp.float32)):
            for _ in range(2):
                scratch += [pltpu.VMEM((L if c[3] else 1, tall, c[2]), dtype) for c in chunks]
            for slots in (L, L + 1):
                scratch += [pltpu.VMEM((slots, 1 if c[3] else 2, tall, c[2]), dtype) for c in chunks]
        scratch += [pltpu.VMEM((L, 2, rows, c[2]), bf16) for c in chunks]
        scratch += [
            pltpu.VMEM((1, n * rows), jnp.float32),
            pltpu.VMEM((n, 1, n * rows), jnp.float32),
            pltpu.VMEM((n, 1, wide_norm), jnp.float32),
        ]
        sem = pltpu.SemaphoreType.DMA
        scratch += [
            sem((2 * count + 15,)),
            sem((2, 2, count, L)),
            sem((2, 2, count, L + 1)),
            sem((2, count, L + 1)),
            sem((2, count, L)),
            sem((2, 2, n)),
        ]
        anywhere = pl.BlockSpec(memory_space=pl.ANY)
        vmem = pl.BlockSpec(memory_space=pltpu.VMEM)
        with jax.sharding.use_abstract_mesh(mesh.abstract_mesh):
            outs = pl.pallas_call(
                functools.partial(kernel, n, chunks),
                out_shape=out_shape,
                in_specs=[anywhere] * 21,
                out_specs=[vmem] * 21,
                scratch_shapes=scratch,
                compiler_params=pltpu.CompilerParams(
                    collective_id=0, has_side_effects=True, vmem_limit_bytes=48 * 2**20
                ),
            )(*grads, *weights, *moments)
            total = len(outs)
            outs = pl.pallas_call(
                functools.partial(hand_on, total),
                out_shape=[jax.ShapeDtypeStruct(o.shape, o.dtype) for o in out_shape],
                in_specs=[vmem] * total,
                out_specs=[anywhere] * total,
                scratch_shapes=[sem((total,))],
                compiler_params=pltpu.CompilerParams(vmem_limit_bytes=2**20),
            )(*outs)
        outs = list(outs)
        for i in (2, 3, 4, 8, 15):
            outs[i] = outs[i].T
        outs[6] = outs[6].reshape(-1).astype(jnp.bfloat16)
        outs[13] = outs[13].reshape(-1)
        outs[20] = outs[20].reshape(-1)
        return tuple(outs)

    row, col, vec = P("data", "width"), P("width", "data"), P("data")
    part = (row, col, row, row, row, col, vec)
    return jax.shard_map(
        on_device,
        mesh=mesh,
        in_specs=(
            P("data", None, "width"),
            P("data", "width", None),
            P("data", None, "width"),
            P("data", None, "width"),
            P("data", None, "width"),
            P("data", "width", None),
            P("data", None),
        )
        + part
        + part,
        out_specs=(
            P(None, "width"),
            P("width", None),
            P(None, "width"),
            P(None, "width"),
            P(None, "width"),
            P("width", None),
            P(),
        )
        + part
        + part,
        check_vma=False,
    )
```

```python
import functools

import jax
import jax.numpy as jnp
from jax import lax
from jax.experimental import pallas as pl
from jax.experimental.pallas import tpu as pltpu
from jax.sharding import PartitionSpec as P

learn_rate = 0.05
hold_rate = 0.9
LANES = 128
SUB = 8
LOW, REACH = -125.0, 251.0
TINY = 1e-30


PLAN = [
    ("up", 2, 0),
    ("up", 2, 1),
    ("down", 2, 1),
    ("down", 2, 1),
    ("vm", 1, 0),
    ("qk", 3, 1),
    ("vm", 2, 1),
    ("down", 2, 0),
    ("up", 2, 1),
]
ORDERS = [
    [
        (0, 0, 0), (2, 0, 0), (2, 0, 1), (0, 2, 0), (1, 2, 0), (1, 2, 2), (0, 4, 0), (0, 1, 0),
        (2, 4, 0), (1, 1, 0), (0, 3, 0), (0, 5, 0), (2, 2, 0), (1, 2, 1), (1, 1, 1), (1, 3, 2),
        (2, 1, 0), (1, 3, 1), (1, 3, 0), (1, 1, 3), (1, 1, 2), (1, 5, 0), (2, 0, 2), (1, 5, 2),
        (2, 2, 1), (1, 5, 1), (1, 2, 3), (2, 4, 1), (2, 1, 1), (0, 8, 0), (0, 6, 0), (1, 8, 3),
        (2, 3, 0), (2, 2, 2), (2, 3, 1), (1, 3, 3), (0, 7, 0), (2, 1, 2), (4, 1, 0), (3, 0, 0),
        (1, 8, 2), (2, 3, 2), (2, 5, 0), (2, 5, 1), (1, 6, 1), (2, 4, 2), (2, 7, 0), (1, 6, 0),
        (3, 4, 0), (4, 2, 0), (1, 8, 0), (4, 0, 0), (1, 6, 2), (2, 5, 2), (6, 2, -2), (6, 3, -1),
        (2, 7, 1), (2, 6, 0), (1, 5, 3), (6, 1, -1), (1, 8, 1), (5, 0, 0), (2, 6, 1), (2, 7, 2),
        (2, 8, 0), (6, 5, -1), (4, 4, 0), (4, 3, 0), (1, 6, 3), (5, 4, 0), (3, 7, 0), (6, 1, -3),
        (2, 6, 2), (6, 2, -3), (4, 5, 0), (6, 0, -3), (2, 8, 1), (6, 2, -1), (6, 3, -2), (4, 6, 0),
        (6, 0, -2), (4, 7, 0), (2, 8, 2), (6, 3, -3), (6, 5, -2), (4, 8, 0), (6, 6, -1), (6, 1, -2),
        (5, 7, 0), (6, 7, -1), (6, 4, -1), (6, 6, -2), (6, 0, -1), (7, 3, 0), (6, 8, -1), (7, 1, 0),
        (6, 5, -3), (7, 0, 0), (6, 4, -3), (7, 2, 0), (6, 6, -3), (6, 8, -2), (6, 8, -3), (7, 5, 0),
        (6, 4, -2), (7, 6, 0), (7, 4, 0), (7, 8, 0), (6, 7, -2), (6, 7, -3), (7, 7, 0),
    ],
    [
        (0, 1, 0), (1, 1, 1), (0, 0, 0), (0, 3, 0), (1, 1, 3), (1, 1, 2), (0, 2, 0), (0, 5, 0),
        (1, 2, 0), (1, 3, 0), (1, 2, 1), (1, 1, 0), (2, 0, 0), (0, 6, 0), (1, 2, 3), (2, 0, 1),
        (0, 4, 0), (1, 3, 2), (2, 2, 0), (1, 2, 2), (2, 1, 0), (1, 3, 1), (2, 0, 2), (1, 5, 0),
        (2, 4, 0), (1, 6, 2), (3, 0, 0), (2, 1, 2), (2, 2, 1), (1, 3, 3), (2, 2, 2), (0, 7, 0),
        (2, 1, 1), (2, 4, 2), (2, 3, 0), (1, 5, 3), (1, 5, 2), (4, 2, 0), (2, 3, 1), (4, 0, 0),
        (1, 5, 1), (2, 4, 1), (2, 3, 2), (6, 1, 1), (4, 1, 0), (6, 2, -1), (4, 3, 0), (2, 5, 0),
        (5, 0, 0), (6, 1, -2), (0, 8, 0), (1, 6, 0), (3, 4, 0), (2, 5, 1), (6, 1, -1), (2, 5, 2),
        (6, 0, -1), (6, 2, 1), (2, 7, 0), (4, 5, 0), (2, 7, 1), (4, 4, 0), (6, 3, -1), (1, 6, 1),
        (6, 2, -2), (2, 7, 2), (1, 8, 0), (6, 0, 1), (2, 6, 0), (6, 5, -1), (2, 6, 1), (3, 7, 0),
        (1, 6, 3), (5, 4, 0), (6, 0, -2), (2, 8, 0), (2, 6, 2), (6, 3, 1), (1, 8, 2), (6, 4, 1),
        (6, 4, -1), (7, 0, 0), (1, 8, 1), (4, 7, 0), (4, 6, 0), (1, 8, 3), (6, 5, 1), (6, 3, -2),
        (2, 8, 2), (6, 6, -1), (2, 8, 1), (6, 4, -2), (6, 6, 1), (5, 7, 0), (4, 8, 0), (6, 5, -2),
        (7, 4, 0), (6, 6, -2), (6, 8, 1), (6, 8, -1), (6, 7, 1), (6, 8, -2), (6, 7, -1), (7, 2, 0),
        (7, 3, 0), (6, 7, -2), (7, 7, 0), (7, 8, 0), (7, 1, 0), (7, 6, 0), (7, 5, 0),
    ],
]


def round_up(value, unit):
    return -(-value // unit) * unit


def turn(block):
    rows, cols = block.shape
    tall, wide = round_up(rows, LANES), round_up(cols, LANES)
    if wide != cols:
        block = jnp.concatenate([block, jnp.zeros((rows, wide - cols), block.dtype)], axis=1)
    if tall != rows:
        block = jnp.concatenate([block, jnp.zeros((tall - rows, wide), block.dtype)], axis=0)
    return block.T[:cols, :rows]


def encode(x):
    limit = jnp.maximum(jnp.max(jnp.abs(x), axis=0, keepdims=True), TINY)
    size = jnp.exp2(jnp.abs(x) * (REACH / limit) + LOW)
    return jnp.where(x < 0.0, -size, size).astype(jnp.bfloat16), limit


def decode(code, limit):
    code = code.astype(jnp.float32)
    rate = limit * (1.0 / REACH)
    size = jnp.log2(jnp.abs(code)) * rate - LOW * rate
    return jnp.where(code < 0.0, -size, size)


PREP, START, STEP, HALF, FINISH, PAIR, HOP, END = range(8)


def make_chunks(cols, heads, plan):
    room = {"up": cols, "down": cols, "vm": 2 * heads, "qk": 2 * heads}
    if sum(room.values()) != LANES * sum(p[1] for p in plan):
        plan = [("up", cols // LANES, 1), ("vm", 2 * heads // LANES, 0), ("down", cols // LANES, 1)]
        plan += [("qk", 2 * heads // LANES, 0)]
    at = dict.fromkeys(room, 0)
    chunks = []
    for kind, tiles, y_first in plan:
        chunks.append((kind, at[kind], tiles * LANES, bool(y_first)))
        at[kind] += tiles * LANES
    return chunks


def plain_order(L, chunks):
    events = []
    for c, (_, _, _, y_first) in enumerate(chunks):
        time = 4 * c

        def add(kind, arg=0):
            events.append((time, len(events), (kind, c, arg)))

        add(PREP)
        if y_first:
            for i in range(L):
                add(START, i)
            time += 4
        for i in range(L - 1):
            add(STEP, i)
            time += 2
        if not y_first:
            add(HALF)
            time += 4
        add(FINISH)
        if not y_first:
            time += 4
            add(PAIR)
        for h in range(1, L):
            time += 4
            add(HOP, h)
            add(HOP, -h)
        time += 4
        add(END)
    return [e[2] for e in sorted(events)]


def pick(cond, one, two):
    if isinstance(cond, bool):
        return one if cond else two
    return jnp.where(cond, one, two)


def when(cond, body):
    if not isinstance(cond, bool):
        pl.when(cond)(body)
    elif cond:
        body()


def start(copies):
    for copy in copies:
        copy.start()


def wait_recv(copies):
    for copy in copies:
        copy.wait_recv()


def wait_send(copies):
    for copy in copies:
        copy.wait_send()


def remote(src, dst, sems, send_slot, recv_slot, there):
    return pltpu.make_async_remote_copy(
        src_ref=src,
        dst_ref=dst,
        send_sem=sems.at[(0,) + send_slot],
        recv_sem=sems.at[(1,) + recv_slot],
        device_id={"data": there},
        device_id_type=pl.DeviceIdType.MESH,
    )


def update(total, weight, moment, mean_rate):
    mean = total * mean_rate
    state = hold_rate * moment + (1.0 - hold_rate) * mean * mean
    return weight - learn_rate * mean * lax.rsqrt(state + 1e-06), state


def kernel(n, chunks, orders, *refs):
    refs = list(refs)
    take = lambda count: [refs.pop(0) for _ in range(count)]
    grads = dict(zip(("up", "down", "query", "key", "value", "mixed", "norm"), take(7)))
    given = take(14)
    c_up, c_down, c_query, c_key, c_value, c_mixed, c_norm = take(7)
    n_up, n_down, n_query, n_key, n_value, n_mixed, n_norm = take(7)
    s_up, s_down, s_query, s_key, s_value, s_mixed, s_norm = take(7)
    near = take(14)
    w_up, w_down, w_query, w_key, w_value, w_mixed, w_norm = near[:7]
    m_up, m_down, m_query, m_key, m_value, m_mixed, m_norm = near[7:]
    pair = {kind: take(4) for kind in ("qk", "vm")}
    count = len(chunks)
    L = n // 2
    raw = take(count)
    part = take(count)
    ysend = take(count)
    yhold = take(count)
    zsend = take(count)
    zhold = take(count)
    ysend_range, yhold_range, zsend_range, zhold_range = take(count), take(count), take(count), take(count)
    copies = take(count)
    g_norm, norm_hold, norm_copy = take(3)
    load_sem, y_sems, z_sems, ag_sems, ay_sems, norm_sems = take(6)

    rows = part[0].shape[-2]
    heads = w_query.shape[-1]
    mean_rate = n ** (-0.5)
    me = lax.axis_index("data")
    y, z = me % 2, me // 2
    other = 1 - y
    partner = me + 1 - 2 * y

    loads, small, at = [], [], 0
    for chunk, (kind, first, wide, _) in enumerate(chunks):
        if kind == "up":
            moves = [(grads["up"].at[:, :, pl.ds(first, wide)], part[chunk])]
        elif kind == "down":
            moves = [(grads["down"].at[pl.ds(first, wide)], raw[chunk])]
        else:
            moves = []
            for k, name in enumerate(("query", "key") if kind == "qk" else ("value", "mixed")):
                low, high = max(first, k * heads), min(first + wide, (k + 1) * heads)
                if low < high:
                    src = grads[name].at[pl.ds(low - k * heads, high - low)]
                    moves.append((src, raw[chunk].at[pl.ds(low - first, high - low)]))
        group = []
        for src, dst in moves:
            group.append(pltpu.make_async_copy(src, dst, load_sem.at[at]))
            at += 1
        loads.append(group)
    for src, dst in [(grads["norm"], g_norm)] + list(zip(given, near)):
        small.append(pltpu.make_async_copy(src, dst, load_sem.at[at]))
        at += 1
    for k, group in enumerate(loads):
        start(group)
        if k == 1:
            start(small[:1])
    start(small[1:])

    barrier = pltpu.get_barrier_semaphore()
    for step in range(1, n):
        pl.semaphore_signal(
            barrier, inc=1, device_id={"data": (me + step) % n}, device_id_type=pl.DeviceIdType.MESH
        )

    def norm_copies(give):
        src, dst = (g_norm, norm_hold) if give else (norm_copy.at[me], norm_copy)
        sets = [((0 if give else 1, step), (me + step) % n) for step in range(1, n)]
        return [remote(src, dst.at[me], norm_sems, slot, slot, there) for slot, there in sets]

    def norm_arrivals(give):
        hold = norm_hold if give else norm_copy
        for step in range(1, n):
            spot, slot = hold.at[(me + n - step) % n], (0 if give else 1, step)
            remote(spot, spot, norm_sems, slot, slot, partner).wait_recv()

    def norm_start():
        small[0].wait()
        norm_hold[me] = g_norm[...]
        start(norm_copies(True))

    def norm_update():
        norm_arrivals(True)
        total = norm_hold[0]
        for d in range(1, n):
            total = total + norm_hold[d]
        own = total[:, :rows]
        for d in range(1, n):
            own = jnp.where(me == d, total[:, d * rows : (d + 1) * rows], own)
        new, state = update(own, w_norm[...], m_norm[...], mean_rate)
        n_norm[...] = new
        s_norm[...] = state
        wide = norm_copy.shape[-1]
        if wide != rows:
            new = jnp.concatenate([new, jnp.zeros((1, wide - rows), jnp.float32)], axis=1)
        norm_copy[me] = new
        start(norm_copies(False))

    def norm_end():
        norm_arrivals(False)
        got = [norm_copy[d][:, :rows] for d in range(n)]
        c_norm[...] = jnp.concatenate(got, axis=1)
        for give in (True, False):
            wait_send(norm_copies(give))

    def smalls():
        for load in small[1:]:
            load.wait()
        pair["qk"][0][...] = jnp.concatenate([w_query[...], w_key[...]], axis=1)
        pair["qk"][1][...] = jnp.concatenate([m_query[...], m_key[...]], axis=1)
        pair["vm"][0][...] = jnp.concatenate([w_value[...], turn(w_mixed[...])], axis=1)
        pair["vm"][1][...] = jnp.concatenate([m_value[...], turn(m_mixed[...])], axis=1)

    def pairs_end(kind):
        new, state = pair[kind][2][...], pair[kind][3][...]
        if kind == "qk":
            n_query[...], n_key[...] = new[:, :heads], new[:, heads:]
            s_query[...], s_key[...] = state[:, :heads], state[:, heads:]
        else:
            n_value[...], s_value[...] = new[:, :heads], state[:, :heads]
            n_mixed[...], s_mixed[...] = turn(new[:, heads:]), turn(state[:, heads:])

    group = 1 if rows % 16 == 0 else 2

    def program(order, zm, mirror):
        forward = 1 - 2 * mirror
        real = lambda place: mirror * (L - 1) + forward * place
        has_near, has_far = zm > 0, zm < L - 1
        from_near, from_far = z + mirror * (L - z), z + (1 - mirror) * (L - z)

        def target(i):
            ahead = L - 1 - zm
            far = pick(i < ahead, L - 1 - i, i - ahead)
            back = pick(i < zm, i, L - 1 - (i - zm))
            return pick(2 * zm < L, far, back)

        def y_copy(chunk, slot):
            pairs = ((ysend, yhold), (ysend_range, yhold_range))
            return [
                remote(src[chunk].at[slot], dst[chunk].at[slot], y_sems, (k, chunk, slot), (k, chunk, slot), partner)
                for k, (src, dst) in enumerate(pairs)
            ]

        def y_value(chunk, slot):
            return decode(yhold[chunk][slot], yhold_range[chunk][slot])

        def y_code(chunk, slot, value):
            ysend[chunk][slot], ysend_range[chunk][slot] = encode(value)
            start(y_copy(chunk, slot))

        def z_copy(chunk, place):
            ahead = place > zm
            there, t = pick(ahead, zm + 1, zm - 1), real(place)
            leftward = pick(ahead, mirror, 1 - mirror)
            slot = pick(there == place, t + leftward * (L - t), t)
            pairs = ((zsend, zhold), (zsend_range, zhold_range))
            return [
                remote(
                    src[chunk].at[t],
                    dst[chunk].at[slot],
                    z_sems,
                    (k, chunk, t),
                    (k, chunk, slot),
                    2 * real(there) + y,
                )
                for k, (src, dst) in enumerate(pairs)
            ]

        def z_wait(chunk, slot):
            for k, hold in enumerate((zhold, zhold_range)):
                spot = hold[chunk].at[slot]
                remote(spot, spot, z_sems, (k, chunk, slot), (k, chunk, slot), partner).wait_recv()

        def z_value(chunk, slot, k):
            return decode(zhold[chunk][slot, k], zhold_range[chunk][slot, k])

        def prep(chunk, _):
            for load in loads[chunk]:
                load.wait()
            if chunks[chunk][0] == "up":
                return
            for j in range(chunks[chunk][2] // LANES):
                block = turn(raw[chunk][j * LANES : (j + 1) * LANES, :])
                part[chunk][:, :, j * LANES : (j + 1) * LANES] = block.reshape(n, rows, LANES)

        def start_y(chunk, i):
            t = z if i == L - 1 else real(target(i))
            y_code(chunk, t, part[chunk][2 * t + other])

        def step_z(chunk, i):
            place = target(i)
            t = real(place)
            held = pick(place > zm, has_near, has_far)
            if chunks[chunk][3]:
                wait_recv(y_copy(chunk, t))
                owners = (2 * t + y,)
            else:
                owners = (2 * t, 2 * t + 1)

            def own(owner):
                value = part[chunk][owner]
                return value + y_value(chunk, t) if chunks[chunk][3] else value

            def with_held():
                z_wait(chunk, t)
                for k, owner in enumerate(owners):
                    total = own(owner) + z_value(chunk, t, k)
                    zsend[chunk][t, k], zsend_range[chunk][t, k] = encode(total)

            def without():
                for k, owner in enumerate(owners):
                    zsend[chunk][t, k], zsend_range[chunk][t, k] = encode(own(owner))

            when(held, with_held)
            when((not held) if isinstance(held, bool) else jnp.logical_not(held), without)
            start(z_copy(chunk, place))

        def add_held(chunk, owners):
            for there, slot in ((has_near, from_near), (has_far, from_far)):

                def body():
                    z_wait(chunk, slot)
                    for k, owner in enumerate(owners):
                        part[chunk][owner] = part[chunk][owner] + z_value(chunk, slot, k)

                when(there, body)

        def half_z(chunk, _):
            add_held(chunk, (2 * z, 2 * z + 1))
            y_code(chunk, 0, part[chunk][2 * z + other])

        def finish(chunk, _):
            kind, first, wide, y_first = chunks[chunk]
            if y_first:
                add_held(chunk, (me,))
            slot = z if y_first else 0
            wait_recv(y_copy(chunk, slot))
            total = part[chunk][me] + y_value(chunk, slot)
            if kind == "up":
                weight, moment, new_out, state_out = w_up, m_up, n_up, s_up
            elif kind == "down":
                weight, moment, new_out, state_out = w_down, m_down, n_down, s_down
            else:
                weight, moment, new_out, state_out = pair[kind]
            cols = slice(first, first + wide)
            new, state = update(total, weight[:, cols], moment[:, cols], mean_rate)
            copies[chunk][z, y] = new.astype(jnp.bfloat16)
            if y_first:
                spread(chunk, z, True, True)
                share(chunk, z).start()
            else:
                whole(chunk, y).start()
            new_out[:, cols] = new
            state_out[:, cols] = state

        def whole(chunk, side):
            spot = copies[chunk].at[z, side]
            return remote(spot, spot, ay_sems, (chunk, 0), (chunk, 0), partner)

        def share(chunk, s, side=y):
            spot = copies[chunk].at[s, side]
            return remote(spot, spot, ay_sems, (chunk, s), (chunk, s), partner)

        def line(chunk, s, ahead, slot):
            spot = copies[chunk].at[s, y] if chunks[chunk][3] else copies[chunk].at[s]
            there = 2 * real(zm + 1 if ahead else zm - 1) + y
            return remote(spot, spot, ag_sems, (chunk, slot), (chunk, s), there)

        def spread(chunk, s, far, close):
            if far:
                when(has_far, lambda: line(chunk, s, True, s).start())
            if close:
                when(has_near, lambda: line(chunk, s, False, L if far else s).start())

        def start_pair(chunk, _):
            whole(chunk, other).wait_recv()
            spread(chunk, z, True, True)

        def hop(chunk, h):
            place = zm - h

            def body():
                s = real(place)
                line(chunk, s, h > 0, s).wait_recv()
                spread(chunk, s, h > 0, h < 0)
                if chunks[chunk][3]:
                    share(chunk, s).start()

            when(place >= 0 if h > 0 else place < L, body)

        def drain(chunk):
            y_first = chunks[chunk][3]
            for t in range(L if y_first else 1):
                wait_send(y_copy(chunk, t))
            for i in range(L - 1):
                wait_send(z_copy(chunk, target(i)))
            if y_first:
                for s in range(L):
                    share(chunk, s).wait_send()
            else:
                whole(chunk, y).wait_send()
            when(has_far, lambda: line(chunk, z, True, z).wait_send())
            when(has_near, lambda: line(chunk, z, False, L).wait_send())
            for h in range(1, L):
                for place, ahead, on in ((zm - h, True, has_far), (zm + h, False, has_near)):
                    inside = place >= 0 if ahead else place < L
                    both = (inside and on) if isinstance(on, bool) else jnp.logical_and(inside, on)
                    when(both, lambda: line(chunk, real(place), ahead, real(place)).wait_send())

        def end(chunk, _):
            kind, first, wide, y_first = chunks[chunk]
            if y_first:
                for s in range(L):
                    share(chunk, s, other).wait_recv()
            if kind == "up":
                for d in range(0, n, group):
                    got = [copies[chunk][(d + i) // 2, (d + i) % 2] for i in range(group)]
                    if group > 1:
                        got = [jnp.concatenate([g.astype(jnp.float32) for g in got], axis=0).astype(jnp.bfloat16)]
                    c_up[d * rows : (d + group) * rows, first : first + wide] = got[0]
                return
            for j in range(wide // LANES):
                value = copies[chunk][:, :, :, j * LANES : (j + 1) * LANES].astype(jnp.float32)
                value = turn(value.reshape(n * rows, LANES)).astype(jnp.bfloat16)
                low = first + j * LANES
                if kind == "down":
                    c_down[low : low + LANES, :] = value
                    continue
                for k, out in enumerate((c_query, c_key) if kind == "qk" else (c_value, c_mixed)):
                    top, bottom = max(low, k * heads), min(low + LANES, (k + 1) * heads)
                    if top < bottom:
                        out[top - k * heads : bottom - k * heads, :] = value[top - low : bottom - low]

        bodies = [prep, start_y, step_z, half_z, finish, start_pair, hop, end]
        first_finish = [e[0] for e in order].index(FINISH)
        marks = {first_finish: [smalls]}
        for place, body in ((1, norm_update), (2, norm_end)):
            marks.setdefault(first_finish + place * (len(order) - first_finish) // 3, []).append(body)
        barrier_done, late = False, []
        left = {kind: [c[0] for c in chunks].count(kind) for kind in ("up", "down", "vm", "qk")}
        for k, (kind, chunk, arg) in enumerate(order):
            if kind != PREP and not barrier_done:
                pl.semaphore_wait(barrier, n - 1)
                barrier_done = True
                late_norm = True
            for body in marks.get(k, []):
                body()
            bodies[kind](chunk, arg)
            if kind == FINISH:
                left[chunks[chunk][0]] -= 1
                if chunks[chunk][0] in pair and left[chunks[chunk][0]] == 0:
                    pairs_end(chunks[chunk][0])
            if kind == START + 0 or kind == STEP:
                if barrier_done and late_norm:
                    norm_start()
                    late_norm = False
            if kind == END:
                late.append(chunk)
                if len(late) > 2:
                    drain(late.pop(0))
        for chunk in late:
            drain(chunk)

    if orders:
        place = jnp.minimum(z, L - 1 - z)
        mirror = (2 * z) // L
        for zm, order in enumerate(orders):
            pl.when(place == zm)(functools.partial(program, order, zm, mirror))
    else:
        program(plain_order(L, chunks), z, 0)


def hand_on(count, *refs):
    given, out, sem = refs[:count], refs[count : 2 * count], refs[2 * count]
    writes = [pltpu.make_async_copy(given[i], out[i], sem.at[i]) for i in range(count)]
    for write in writes:
        write.start()
    for write in writes:
        write.wait()


def solution(mesh):
    n = mesh.shape["data"]
    L = n // 2

    def on_device(*args):
        grads, weights, moments = args[:7], args[7:14], args[14:]
        rows = weights[0].shape[0]
        cols = grads[0].shape[2]
        grads = [g[0].T if i in (2, 3, 4) else g[0] for i, g in enumerate(grads[:6])] + [grads[6]]
        grads[0] = grads[0].reshape(n, rows, cols)
        heads = grads[2].shape[0]
        weights = list(weights[:6]) + [weights[6].reshape(1, rows)]
        moments = list(moments[:6]) + [moments[6].reshape(1, rows)]
        weights[1], moments[1] = weights[1].T, moments[1].T
        chunks = make_chunks(cols, heads, PLAN)
        orders = ORDERS if len(ORDERS) == L // 2 and len(chunks) == len(PLAN) else None
        count = len(chunks)
        wide_norm = round_up(rows, LANES)
        copy_shapes = [(n * rows, cols), grads[1].shape] + [g.shape for g in grads[2:6]]
        out_shape = (
            [pltpu.VMEM(s, jnp.bfloat16) for s in copy_shapes]
            + [pltpu.VMEM((1, n * rows), jnp.float32)]
            + [pltpu.VMEM(w.shape, jnp.float32) for w in weights] * 2
        )
        scratch = [pltpu.VMEM(w.shape, jnp.float32) for w in weights + moments]
        scratch += [pltpu.VMEM((rows, 2 * heads), jnp.float32)] * 8
        bf16 = jnp.bfloat16
        scratch += [pltpu.VMEM((c[2], n * rows) if c[0] != "up" else (SUB, LANES), jnp.float32) for c in chunks]
        scratch += [pltpu.VMEM((n, rows, c[2]), jnp.float32) for c in chunks]
        for tall, dtype in ((rows, bf16), (1, jnp.float32)):
            for _ in range(2):
                scratch += [pltpu.VMEM((L if c[3] else 1, tall, c[2]), dtype) for c in chunks]
            for slots in (L, L + 1):
                scratch += [pltpu.VMEM((slots, 1 if c[3] else 2, tall, c[2]), dtype) for c in chunks]
        scratch += [pltpu.VMEM((L, 2, rows, c[2]), bf16) for c in chunks]
        scratch += [
            pltpu.VMEM((1, n * rows), jnp.float32),
            pltpu.VMEM((n, 1, n * rows), jnp.float32),
            pltpu.VMEM((n, 1, wide_norm), jnp.float32),
        ]
        sem = pltpu.SemaphoreType.DMA
        scratch += [
            sem((2 * count + 15,)),
            sem((2, 2, count, L)),
            sem((2, 2, count, L + 1)),
            sem((2, count, L + 1)),
            sem((2, count, L)),
            sem((2, 2, n)),
        ]
        anywhere = pl.BlockSpec(memory_space=pl.ANY)
        hbm = pl.BlockSpec(memory_space=pltpu.HBM)
        vmem = pl.BlockSpec(memory_space=pltpu.VMEM)
        with jax.sharding.use_abstract_mesh(mesh.abstract_mesh):
            outs = pl.pallas_call(
                functools.partial(kernel, n, chunks, orders),
                out_shape=out_shape,
                in_specs=[hbm] * 21,
                out_specs=[vmem] * 21,
                scratch_shapes=scratch,
                compiler_params=pltpu.CompilerParams(
                    collective_id=0, has_side_effects=True, vmem_limit_bytes=48 * 2**20
                ),
            )(*[pltpu.with_memory_space_constraint(a, pltpu.HBM) for a in grads + weights + moments])
            total = len(outs)
            outs = pl.pallas_call(
                functools.partial(hand_on, total),
                out_shape=[jax.ShapeDtypeStruct(o.shape, o.dtype) for o in out_shape],
                in_specs=[vmem] * total,
                out_specs=[anywhere] * total,
                scratch_shapes=[sem((total,))],
                compiler_params=pltpu.CompilerParams(vmem_limit_bytes=2**20),
            )(*outs)
        outs = list(outs)
        for i in (2, 3, 4, 8, 15):
            outs[i] = outs[i].T
        outs[6] = outs[6].reshape(-1).astype(jnp.bfloat16)
        outs[13] = outs[13].reshape(-1)
        outs[20] = outs[20].reshape(-1)
        return tuple(outs)

    row, col, vec = P("data", "width"), P("width", "data"), P("data")
    part = (row, col, row, row, row, col, vec)
    return jax.shard_map(
        on_device,
        mesh=mesh,
        in_specs=(
            P("data", None, "width"),
            P("data", "width", None),
            P("data", None, "width"),
            P("data", None, "width"),
            P("data", None, "width"),
            P("data", "width", None),
            P("data", None),
        )
        + part
        + part,
        out_specs=(
            P(None, "width"),
            P("width", None),
            P(None, "width"),
            P(None, "width"),
            P(None, "width"),
            P("width", None),
            P(),
        )
        + part
        + part,
        check_vma=False,
    )
```

```python
import functools

import jax
import jax.numpy as jnp
from jax import lax
from jax.experimental import pallas as pl
from jax.experimental.pallas import tpu as pltpu
from jax.sharding import PartitionSpec as P

learn_rate = 0.05
hold_rate = 0.9
LANES = 128
SUB = 8
NORM = 6
LOW, REACH = -125.0, 251.0
TINY = 1e-30


PLAN = [
    ("up", 2, 0),
    ("up", 2, 1),
    ("down", 2, 1),
    ("down", 2, 1),
    ("vm", 1, 0),
    ("qk", 3, 1),
    ("vm", 2, 1),
    ("down", 2, 0),
    ("up", 2, 1),
]
ORDERS = [
    [
        (0, 0, 0), (0, 1, 0), (2, 0, 0), (1, 1, 1), (1, 1, 0), (0, 2, 0), (0, 5, 0), (1, 1, 2),
        (1, 5, 3), (1, 2, 1), (2, 0, 1), (0, 3, 0), (1, 3, 0), (2, 1, 1), (1, 2, 0), (1, 3, 1),
        (0, 4, 0), (2, 1, 0), (2, 0, 2), (2, 4, 1), (2, 1, 2), (0, 8, 0), (1, 2, 2), (2, 2, 1),
        (0, 6, 0), (1, 1, 3), (1, 5, 1), (1, 6, 0), (0, 7, 0), (1, 3, 2), (2, 3, 0), (2, 2, 0),
        (2, 4, 0), (1, 5, 0), (2, 2, 2), (2, 7, 0), (1, 8, 2), (2, 6, 0), (3, 0, 0), (1, 6, 1),
        (2, 3, 2), (2, 3, 1), (1, 8, 3), (1, 5, 2), (2, 5, 1), (1, 8, 0), (4, 0, 0), (1, 6, 2),
        (2, 5, 0), (1, 6, 3), (2, 4, 2), (4, 1, 0), (1, 8, 1), (1, 2, 3), (1, 3, 3), (2, 5, 2),
        (2, 7, 1), (5, 0, 0), (6, 1, -2), (2, 6, 1), (6, 3, -1), (6, 0, -1), (3, 4, 0), (4, 2, 0),
        (2, 7, 2), (3, 7, 0), (2, 8, 0), (4, 4, 0), (6, 2, -1), (6, 1, -1), (2, 6, 2), (6, 3, -2),
        (6, 2, -2), (4, 3, 0), (4, 7, 0), (2, 8, 1), (4, 5, 0), (4, 6, 0), (5, 4, 0), (2, 8, 2),
        (6, 1, -3), (5, 7, 0), (6, 5, -1), (6, 0, -2), (4, 8, 0), (6, 4, -1), (6, 4, -2), (6, 2, -3),
        (6, 5, -2), (6, 6, -2), (6, 6, -1), (6, 3, -3), (6, 0, -3), (6, 8, -1), (6, 8, -2), (6, 5, -3),
        (7, 0, 0), (7, 2, 0), (7, 1, 0), (6, 4, -3), (7, 3, 0), (6, 6, -3), (6, 7, -1), (6, 8, -3),
        (6, 7, -3), (7, 5, 0), (7, 6, 0), (7, 4, 0), (6, 7, -2), (7, 7, 0), (7, 8, 0),
    ],
    [
        (0, 1, 0), (1, 1, 1), (1, 1, 0), (0, 0, 0), (0, 3, 0), (0, 2, 0), (0, 5, 0), (1, 3, 0),
        (0, 7, 0), (0, 8, 0), (1, 1, 3), (1, 1, 2), (1, 2, 0), (1, 5, 1), (2, 0, 0), (1, 3, 3),
        (1, 3, 2), (0, 6, 0), (2, 0, 1), (2, 1, 1), (1, 2, 1), (0, 4, 0), (1, 3, 1), (2, 1, 0),
        (3, 0, 0), (2, 4, 1), (1, 2, 3), (2, 0, 2), (1, 2, 2), (4, 1, 0), (2, 2, 1), (2, 3, 0),
        (4, 0, 0), (2, 2, 0), (2, 1, 2), (1, 6, 1), (6, 1, -1), (2, 4, 0), (1, 6, 0), (1, 5, 0),
        (1, 6, 2), (4, 2, 0), (5, 0, 0), (2, 3, 2), (2, 4, 2), (2, 7, 0), (1, 6, 3), (1, 5, 3),
        (2, 2, 2), (2, 3, 1), (1, 5, 2), (6, 0, -1), (6, 2, -1), (2, 6, 0), (2, 5, 1), (2, 5, 0),
        (4, 3, 0), (2, 6, 2), (3, 4, 0), (6, 1, 1), (2, 7, 2), (4, 5, 0), (2, 7, 1), (4, 4, 0),
        (1, 8, 2), (6, 3, -1), (1, 8, 0), (1, 8, 1), (6, 1, -2), (6, 0, 1), (2, 5, 2), (2, 6, 1),
        (5, 4, 0), (6, 5, -1), (6, 2, 1), (6, 0, -2), (2, 8, 0), (3, 7, 0), (1, 8, 3), (4, 6, 0),
        (6, 4, -1), (6, 3, 1), (2, 8, 2), (2, 8, 1), (6, 5, 1), (6, 2, -2), (6, 6, 1), (7, 1, 0),
        (4, 7, 0), (6, 6, -1), (6, 3, -2), (6, 4, 1), (4, 8, 0), (6, 5, -2), (6, 6, -2), (6, 7, 1),
        (6, 4, -2), (6, 8, -1), (6, 8, 1), (5, 7, 0), (6, 8, -2), (6, 7, -2), (6, 7, -1), (7, 7, 0),
        (7, 2, 0), (7, 4, 0), (7, 0, 0), (7, 8, 0), (7, 5, 0), (7, 6, 0), (7, 3, 0),
    ],
]


def round_up(value, unit):
    return -(-value // unit) * unit


def turn(block):
    rows, cols = block.shape
    tall, wide = round_up(rows, LANES), round_up(cols, LANES)
    if wide != cols:
        block = jnp.concatenate([block, jnp.zeros((rows, wide - cols), block.dtype)], axis=1)
    if tall != rows:
        block = jnp.concatenate([block, jnp.zeros((tall - rows, wide), block.dtype)], axis=0)
    return block.T[:cols, :rows]


def encode(x):
    limit = jnp.maximum(jnp.max(jnp.abs(x), axis=0, keepdims=True), TINY)
    size = jnp.exp2(jnp.abs(x) * (REACH / limit) + LOW)
    return jnp.where(x < 0.0, -size, size).astype(jnp.bfloat16), limit


def decode(code, limit):
    code = code.astype(jnp.float32)
    rate = limit * (1.0 / REACH)
    size = jnp.log2(jnp.abs(code)) * rate - LOW * rate
    return jnp.where(code < 0.0, -size, size)


PREP, START, STEP, HALF, FINISH, PAIR, HOP, END = range(8)


def make_chunks(cols, heads, plan):
    room = {"up": cols, "down": cols, "vm": 2 * heads, "qk": 2 * heads}
    if sum(room.values()) != LANES * sum(p[1] for p in plan):
        plan = [("up", cols // LANES, 1), ("vm", 2 * heads // LANES, 0), ("down", cols // LANES, 1)]
        plan += [("qk", 2 * heads // LANES, 0)]
    at = dict.fromkeys(room, 0)
    chunks = []
    for kind, tiles, y_first in plan:
        chunks.append((kind, at[kind], tiles * LANES, bool(y_first)))
        at[kind] += tiles * LANES
    return chunks


def plain_order(L, chunks):
    events = []
    for c, (_, _, _, y_first) in enumerate(chunks):
        time = 4 * c

        def add(kind, arg=0):
            events.append((time, len(events), (kind, c, arg)))

        add(PREP)
        if y_first:
            for i in range(L):
                add(START, i)
            time += 4
        for i in range(L - 1):
            add(STEP, i)
            time += 2
        if not y_first:
            add(HALF)
            time += 4
        add(FINISH)
        if not y_first:
            time += 4
            add(PAIR)
        for h in range(1, L):
            time += 4
            add(HOP, h)
            add(HOP, -h)
        time += 4
        add(END)
    return [e[2] for e in sorted(events)]


def pick(cond, one, two):
    if isinstance(cond, bool):
        return one if cond else two
    return jnp.where(cond, one, two)


def when(cond, body):
    if not isinstance(cond, bool):
        pl.when(cond)(body)
    elif cond:
        body()


def start(copies):
    for copy in copies:
        copy.start()


def wait_recv(copies):
    for copy in copies:
        copy.wait_recv()


def wait_send(copies):
    for copy in copies:
        copy.wait_send()


def remote(src, dst, sems, send_slot, recv_slot, there):
    return pltpu.make_async_remote_copy(
        src_ref=src,
        dst_ref=dst,
        send_sem=sems.at[(0,) + send_slot],
        recv_sem=sems.at[(1,) + recv_slot],
        device_id={"data": there},
        device_id_type=pl.DeviceIdType.MESH,
    )


def update(total, weight, moment, mean_rate):
    mean = total * mean_rate
    state = hold_rate * moment + (1.0 - hold_rate) * mean * mean
    return weight - learn_rate * mean * lax.rsqrt(state + 1e-06), state


def kernel(n, chunks, orders, *refs):
    refs = list(refs)
    take = lambda count: [refs.pop(0) for _ in range(count)]
    grads = dict(zip(("up", "down", "query", "key", "value", "mixed", "norm"), take(7)))
    given = take(14)
    c_up, c_down, c_query, c_key, c_value, c_mixed, c_norm = take(7)
    n_up, n_down, n_query, n_key, n_value, n_mixed, n_norm = take(7)
    s_up, s_down, s_query, s_key, s_value, s_mixed, s_norm = take(7)
    near = take(14)
    w_up, w_down, w_query, w_key, w_value, w_mixed, w_norm = near[:7]
    m_up, m_down, m_query, m_key, m_value, m_mixed, m_norm = near[7:]
    pair = {kind: take(4) for kind in ("qk", "vm")}
    count = len(chunks)
    L = n // 2
    raw = take(count)
    part = take(count)
    ysend = take(count)
    yhold = take(count)
    zsend = take(count)
    zhold = take(count)
    ysend_range, yhold_range, zsend_range, zhold_range = take(count), take(count), take(count), take(count)
    copies = take(count)
    g_norm, norm_hold, norm_copy = take(3)
    load_sem, y_sems, z_sems, ag_sems, ay_sems, norm_sems = take(6)

    rows = part[0].shape[-2]
    heads = w_query.shape[-1]
    mean_rate = n ** (-0.5)
    me = lax.axis_index("data")
    y, z = me % 2, me // 2
    other = 1 - y
    partner = me + 1 - 2 * y

    loads, small, at = [], [], 0
    for chunk, (kind, first, wide, _) in enumerate(chunks):
        if kind == "up":
            moves = [(grads["up"].at[:, :, pl.ds(first, wide)], part[chunk])]
        elif kind == "down":
            moves = [(grads["down"].at[pl.ds(first, wide)], raw[chunk])]
        else:
            moves = []
            for k, name in enumerate(("query", "key") if kind == "qk" else ("value", "mixed")):
                low, high = max(first, k * heads), min(first + wide, (k + 1) * heads)
                if low < high:
                    src = grads[name].at[pl.ds(low - k * heads, high - low)]
                    moves.append((src, raw[chunk].at[pl.ds(low - first, high - low)]))
        group = []
        for src, dst in moves:
            group.append(pltpu.make_async_copy(src, dst, load_sem.at[at]))
            at += 1
        loads.append(group)
    for src, dst in [(grads["norm"], g_norm)] + list(zip(given, near)):
        small.append(pltpu.make_async_copy(src, dst, load_sem.at[at]))
        at += 1
    for k, group in enumerate(loads):
        start(group)
        if k == 1:
            start(small[:1])
    start(small[1:])

    barrier = pltpu.get_barrier_semaphore()

    def norm_copies(give):
        src, dst = (g_norm, norm_hold) if give else (norm_copy.at[me], norm_copy)
        sets = [((0 if give else 1, step), (me + step) % n) for step in range(1, n)]
        return [remote(src, dst.at[me], norm_sems, slot, slot, there) for slot, there in sets]

    def norm_arrivals(give):
        hold = norm_hold if give else norm_copy
        for step in range(1, n):
            spot, slot = hold.at[(me + n - step) % n], (0 if give else 1, step)
            remote(spot, spot, norm_sems, slot, slot, partner).wait_recv()

    def norm_start():
        small[0].wait()
        norm_hold[me] = g_norm[...]
        start(norm_copies(True))

    def norm_update():
        norm_arrivals(True)
        total = norm_hold[0]
        for d in range(1, n):
            total = total + norm_hold[d]
        own = total[:, :rows]
        for d in range(1, n):
            own = jnp.where(me == d, total[:, d * rows : (d + 1) * rows], own)
        new, state = update(own, w_norm[...], m_norm[...], mean_rate)
        n_norm[...] = new
        s_norm[...] = state
        wide = norm_copy.shape[-1]
        if wide != rows:
            new = jnp.concatenate([new, jnp.zeros((1, wide - rows), jnp.float32)], axis=1)
        norm_copy[me] = new
        start(norm_copies(False))

    def norm_end():
        norm_arrivals(False)
        got = [norm_copy[d][:, :rows] for d in range(n)]
        c_norm[...] = jnp.concatenate(got, axis=1)
        for give in (True, False):
            wait_send(norm_copies(give))

    def smalls():
        for load in small[1:]:
            load.wait()
        pair["qk"][0][...] = jnp.concatenate([w_query[...], w_key[...]], axis=1)
        pair["qk"][1][...] = jnp.concatenate([m_query[...], m_key[...]], axis=1)
        pair["vm"][0][...] = jnp.concatenate([w_value[...], turn(w_mixed[...])], axis=1)
        pair["vm"][1][...] = jnp.concatenate([m_value[...], turn(m_mixed[...])], axis=1)

    def pairs_end(kind):
        new, state = pair[kind][2][...], pair[kind][3][...]
        if kind == "qk":
            n_query[...], n_key[...] = new[:, :heads], new[:, heads:]
            s_query[...], s_key[...] = state[:, :heads], state[:, heads:]
        else:
            n_value[...], s_value[...] = new[:, :heads], state[:, :heads]
            n_mixed[...], s_mixed[...] = turn(new[:, heads:]), turn(state[:, heads:])

    group = 1 if rows % 16 == 0 else 2

    def program(order, zm, mirror):
        forward = 1 - 2 * mirror
        real = lambda place: mirror * (L - 1) + forward * place
        has_near, has_far = zm > 0, zm < L - 1
        from_near, from_far = z + mirror * (L - z), z + (1 - mirror) * (L - z)

        def target(i):
            ahead = L - 1 - zm
            far = pick(i < ahead, L - 1 - i, i - ahead)
            back = pick(i < zm, i, L - 1 - (i - zm))
            return pick(2 * zm < L, far, back)

        def y_copy(chunk, slot):
            pairs = ((ysend, yhold), (ysend_range, yhold_range))
            return [
                remote(src[chunk].at[slot], dst[chunk].at[slot], y_sems, (k, chunk, slot), (k, chunk, slot), partner)
                for k, (src, dst) in enumerate(pairs)
            ]

        def y_value(chunk, slot):
            return decode(yhold[chunk][slot], yhold_range[chunk][slot])

        def y_code(chunk, slot, value):
            ysend[chunk][slot], ysend_range[chunk][slot] = encode(value)
            start(y_copy(chunk, slot))

        def z_copy(chunk, place):
            ahead = place > zm
            there, t = pick(ahead, zm + 1, zm - 1), real(place)
            leftward = pick(ahead, mirror, 1 - mirror)
            slot = pick(there == place, t + leftward * (L - t), t)
            pairs = ((zsend, zhold), (zsend_range, zhold_range))
            return [
                remote(
                    src[chunk].at[t],
                    dst[chunk].at[slot],
                    z_sems,
                    (k, chunk, t),
                    (k, chunk, slot),
                    2 * real(there) + y,
                )
                for k, (src, dst) in enumerate(pairs)
            ]

        def z_wait(chunk, slot):
            for k, hold in enumerate((zhold, zhold_range)):
                spot = hold[chunk].at[slot]
                remote(spot, spot, z_sems, (k, chunk, slot), (k, chunk, slot), partner).wait_recv()

        def z_value(chunk, slot, k):
            return decode(zhold[chunk][slot, k], zhold_range[chunk][slot, k])

        def prep(chunk, _):
            for load in loads[chunk]:
                load.wait()
            if chunks[chunk][0] == "up":
                return
            for j in range(chunks[chunk][2] // LANES):
                block = turn(raw[chunk][j * LANES : (j + 1) * LANES, :])
                part[chunk][:, :, j * LANES : (j + 1) * LANES] = block.reshape(n, rows, LANES)

        def start_y(chunk, i):
            t = z if i == L - 1 else real(target(i))
            y_code(chunk, t, part[chunk][2 * t + other])

        def step_z(chunk, i):
            place = target(i)
            t = real(place)
            held = pick(place > zm, has_near, has_far)
            if chunks[chunk][3]:
                wait_recv(y_copy(chunk, t))
                owners = (2 * t + y,)
            else:
                owners = (2 * t, 2 * t + 1)

            def own(owner):
                value = part[chunk][owner]
                return value + y_value(chunk, t) if chunks[chunk][3] else value

            def with_held():
                z_wait(chunk, t)
                for k, owner in enumerate(owners):
                    total = own(owner) + z_value(chunk, t, k)
                    zsend[chunk][t, k], zsend_range[chunk][t, k] = encode(total)

            def without():
                for k, owner in enumerate(owners):
                    zsend[chunk][t, k], zsend_range[chunk][t, k] = encode(own(owner))

            when(held, with_held)
            when((not held) if isinstance(held, bool) else jnp.logical_not(held), without)
            start(z_copy(chunk, place))

        def add_held(chunk, owners):
            for there, slot in ((has_near, from_near), (has_far, from_far)):

                def body():
                    z_wait(chunk, slot)
                    for k, owner in enumerate(owners):
                        part[chunk][owner] = part[chunk][owner] + z_value(chunk, slot, k)

                when(there, body)

        def half_z(chunk, _):
            add_held(chunk, (2 * z, 2 * z + 1))
            y_code(chunk, 0, part[chunk][2 * z + other])

        def finish(chunk, _):
            kind, first, wide, y_first = chunks[chunk]
            if y_first:
                add_held(chunk, (me,))
            slot = z if y_first else 0
            wait_recv(y_copy(chunk, slot))
            total = part[chunk][me] + y_value(chunk, slot)
            if kind == "up":
                weight, moment, new_out, state_out = w_up, m_up, n_up, s_up
            elif kind == "down":
                weight, moment, new_out, state_out = w_down, m_down, n_down, s_down
            else:
                weight, moment, new_out, state_out = pair[kind]
            cols = slice(first, first + wide)
            new, state = update(total, weight[:, cols], moment[:, cols], mean_rate)
            copies[chunk][z, y] = new.astype(jnp.bfloat16)
            if y_first:
                spread(chunk, z, True, True)
                share(chunk, z).start()
            else:
                whole(chunk, y).start()
            new_out[:, cols] = new
            state_out[:, cols] = state

        def whole(chunk, side):
            spot = copies[chunk].at[z, side]
            return remote(spot, spot, ay_sems, (chunk, 0), (chunk, 0), partner)

        def share(chunk, s, side=y):
            spot = copies[chunk].at[s, side]
            return remote(spot, spot, ay_sems, (chunk, s), (chunk, s), partner)

        def line(chunk, s, ahead, slot):
            spot = copies[chunk].at[s, y] if chunks[chunk][3] else copies[chunk].at[s]
            there = 2 * real(zm + 1 if ahead else zm - 1) + y
            return remote(spot, spot, ag_sems, (chunk, slot), (chunk, s), there)

        def spread(chunk, s, far, close):
            if far:
                when(has_far, lambda: line(chunk, s, True, s).start())
            if close:
                when(has_near, lambda: line(chunk, s, False, L if far else s).start())

        def start_pair(chunk, _):
            whole(chunk, other).wait_recv()
            spread(chunk, z, True, True)

        def hop(chunk, h):
            place = zm - h

            def body():
                s = real(place)
                line(chunk, s, h > 0, s).wait_recv()
                spread(chunk, s, h > 0, h < 0)
                if chunks[chunk][3]:
                    share(chunk, s).start()

            when(place >= 0 if h > 0 else place < L, body)

        def drain(chunk):
            y_first = chunks[chunk][3]
            for t in range(L if y_first else 1):
                wait_send(y_copy(chunk, t))
            for i in range(L - 1):
                wait_send(z_copy(chunk, target(i)))
            if y_first:
                for s in range(L):
                    share(chunk, s).wait_send()
            else:
                whole(chunk, y).wait_send()
            when(has_far, lambda: line(chunk, z, True, z).wait_send())
            when(has_near, lambda: line(chunk, z, False, L).wait_send())
            for h in range(1, L):
                for place, ahead, on in ((zm - h, True, has_far), (zm + h, False, has_near)):
                    inside = place >= 0 if ahead else place < L
                    both = (inside and on) if isinstance(on, bool) else jnp.logical_and(inside, on)
                    when(both, lambda: line(chunk, real(place), ahead, real(place)).wait_send())

        def end(chunk, _):
            kind, first, wide, y_first = chunks[chunk]
            if y_first:
                for s in range(L):
                    share(chunk, s, other).wait_recv()
            if kind == "up":
                for d in range(0, n, group):
                    got = [copies[chunk][(d + i) // 2, (d + i) % 2] for i in range(group)]
                    if group > 1:
                        got = [jnp.concatenate([g.astype(jnp.float32) for g in got], axis=0).astype(jnp.bfloat16)]
                    c_up[d * rows : (d + group) * rows, first : first + wide] = got[0]
                return
            for j in range(wide // LANES):
                value = copies[chunk][:, :, :, j * LANES : (j + 1) * LANES].astype(jnp.float32)
                value = turn(value.reshape(n * rows, LANES)).astype(jnp.bfloat16)
                low = first + j * LANES
                if kind == "down":
                    c_down[low : low + LANES, :] = value
                    continue
                for k, out in enumerate((c_query, c_key) if kind == "qk" else (c_value, c_mixed)):
                    top, bottom = max(low, k * heads), min(low + LANES, (k + 1) * heads)
                    if top < bottom:
                        out[top - k * heads : bottom - k * heads, :] = value[top - low : bottom - low]

        def greet(there):
            pl.semaphore_signal(
                barrier, inc=1, device_id={"data": there}, device_id_type=pl.DeviceIdType.MESH
            )

        greet(partner)
        when(has_near, lambda: greet(2 * real(zm - 1) + y))
        when(has_far, lambda: greet(2 * real(zm + 1) + y))
        bodies = [prep, start_y, step_z, half_z, finish, start_pair, hop, end]
        first_finish = [e[0] for e in order].index(FINISH)
        marks = {first_finish: [smalls]}
        for place, body in ((1, norm_update), (2, norm_end)):
            marks.setdefault(first_finish + place * (len(order) - first_finish) // 3, []).append(body)
        barrier_done, late = False, []
        left = {kind: [c[0] for c in chunks].count(kind) for kind in ("up", "down", "vm", "qk")}
        for k, (kind, chunk, arg) in enumerate(order):
            if kind != PREP and not barrier_done:
                pl.semaphore_wait(barrier, 1 + pick(has_near, 1, 0) + pick(has_far, 1, 0))
                barrier_done = True
            for body in marks.get(k, []):
                body()
            bodies[kind](chunk, arg)
            if k == first_finish:
                norm_start()
            if kind == FINISH:
                left[chunks[chunk][0]] -= 1
                if chunks[chunk][0] in pair and left[chunks[chunk][0]] == 0:
                    pairs_end(chunks[chunk][0])
            if kind == END:
                late.append(chunk)
                if len(late) > 2:
                    drain(late.pop(0))
        for chunk in late:
            drain(chunk)

    if orders:
        place = jnp.minimum(z, L - 1 - z)
        mirror = (2 * z) // L
        for zm, order in enumerate(orders):
            pl.when(place == zm)(functools.partial(program, order, zm, mirror))
    else:
        program(plain_order(L, chunks), z, 0)


def hand_on(count, *refs):
    given, out, sem = refs[:count], refs[count : 2 * count], refs[2 * count]
    writes = [pltpu.make_async_copy(given[i], out[i], sem.at[i]) for i in range(count) if i != NORM]
    for write in writes:
        write.start()
    out[NORM][...] = given[NORM][...].reshape(-1).astype(jnp.bfloat16)
    for write in writes:
        write.wait()


def solution(mesh):
    n = mesh.shape["data"]
    L = n // 2

    def on_device(*args):
        grads, weights, moments = args[:7], args[7:14], args[14:]
        rows = weights[0].shape[0]
        cols = grads[0].shape[2]
        grads = [g[0].T if i in (2, 3, 4) else g[0] for i, g in enumerate(grads[:6])] + [grads[6]]
        grads[0] = grads[0].reshape(n, rows, cols)
        heads = grads[2].shape[0]
        weights = list(weights[:6]) + [weights[6].reshape(1, rows)]
        moments = list(moments[:6]) + [moments[6].reshape(1, rows)]
        weights[1], moments[1] = weights[1].T, moments[1].T
        chunks = make_chunks(cols, heads, PLAN)
        orders = ORDERS if len(ORDERS) == L // 2 and len(chunks) == len(PLAN) else None
        count = len(chunks)
        wide_norm = round_up(rows, LANES)
        copy_shapes = [(n * rows, cols), grads[1].shape] + [g.shape for g in grads[2:6]]
        out_shape = (
            [pltpu.VMEM(s, jnp.bfloat16) for s in copy_shapes]
            + [pltpu.VMEM((1, n * rows), jnp.float32)]
            + [pltpu.VMEM(w.shape, jnp.float32) for w in weights] * 2
        )
        scratch = [pltpu.VMEM(w.shape, jnp.float32) for w in weights + moments]
        scratch += [pltpu.VMEM((rows, 2 * heads), jnp.float32)] * 8
        bf16 = jnp.bfloat16
        scratch += [pltpu.VMEM((c[2], n * rows) if c[0] != "up" else (SUB, LANES), jnp.float32) for c in chunks]
        scratch += [pltpu.VMEM((n, rows, c[2]), jnp.float32) for c in chunks]
        for tall, dtype in ((rows, bf16), (1, jnp.float32)):
            for _ in range(2):
                scratch += [pltpu.VMEM((L if c[3] else 1, tall, c[2]), dtype) for c in chunks]
            for slots in (L, L + 1):
                scratch += [pltpu.VMEM((slots, 1 if c[3] else 2, tall, c[2]), dtype) for c in chunks]
        scratch += [pltpu.VMEM((L, 2, rows, c[2]), bf16) for c in chunks]
        scratch += [
            pltpu.VMEM((1, n * rows), jnp.float32),
            pltpu.VMEM((n, 1, n * rows), jnp.float32),
            pltpu.VMEM((n, 1, wide_norm), jnp.float32),
        ]
        sem = pltpu.SemaphoreType.DMA
        scratch += [
            sem((2 * count + 15,)),
            sem((2, 2, count, L)),
            sem((2, 2, count, L + 1)),
            sem((2, count, L + 1)),
            sem((2, count, L)),
            sem((2, 2, n)),
        ]
        anywhere = pl.BlockSpec(memory_space=pl.ANY)
        hbm = pl.BlockSpec(memory_space=pltpu.HBM)
        vmem = pl.BlockSpec(memory_space=pltpu.VMEM)
        with jax.sharding.use_abstract_mesh(mesh.abstract_mesh):
            outs = pl.pallas_call(
                functools.partial(kernel, n, chunks, orders),
                out_shape=out_shape,
                in_specs=[hbm] * 21,
                out_specs=[vmem] * 21,
                scratch_shapes=scratch,
                compiler_params=pltpu.CompilerParams(
                    collective_id=0, has_side_effects=True, vmem_limit_bytes=48 * 2**20
                ),
            )(*[pltpu.with_memory_space_constraint(a, pltpu.HBM) for a in grads + weights + moments])
            total = len(outs)
            outs = pl.pallas_call(
                functools.partial(hand_on, total),
                out_shape=[
                    jax.ShapeDtypeStruct((o.size,), bf16) if i == NORM else jax.ShapeDtypeStruct(o.shape, o.dtype)
                    for i, o in enumerate(outs)
                ],
                in_specs=[vmem] * total,
                out_specs=[vmem if i == NORM else anywhere for i in range(total)],
                scratch_shapes=[sem((total,))],
                compiler_params=pltpu.CompilerParams(vmem_limit_bytes=2**20),
            )(*outs)
        outs = list(outs)
        for i in (2, 3, 4, 8, 15):
            outs[i] = outs[i].T
        outs[13] = outs[13].reshape(-1)
        outs[20] = outs[20].reshape(-1)
        return tuple(outs)

    row, col, vec = P("data", "width"), P("width", "data"), P("data")
    part = (row, col, row, row, row, col, vec)
    return jax.shard_map(
        on_device,
        mesh=mesh,
        in_specs=(
            P("data", None, "width"),
            P("data", "width", None),
            P("data", None, "width"),
            P("data", None, "width"),
            P("data", None, "width"),
            P("data", "width", None),
            P("data", None),
        )
        + part
        + part,
        out_specs=(
            P(None, "width"),
            P("width", None),
            P(None, "width"),
            P(None, "width"),
            P(None, "width"),
            P("width", None),
            P(),
        )
        + part
        + part,
        check_vma=False,
    )
```
